128 devices in a mesh: group: 4 (over x_lo, core), bl: 32 (over x_hi, y, z).
Axes of the slice: x: 4 (x_hi: 2, x_lo: 2; x = x_hi * 2 + x_lo), y: 4, z: 4, core: 2. Of those that a mesh axis runs over, the one named last changes fastest.
Arguments:
- visibilities: float32 [2, 2048, 16, 1024], P(None, ('group', 'bl')), parts along dimension 1, may hold values from -400 to 400
- flags: int32 [2048, 8], P(('group', 'bl')), parts along dimension 0, may hold values 0 or 1
Outputs:
- cross_power: float32 [32, 2048, 512], P(None, ('group', 'bl')), parts along dimension 1
- bandpower: float32 [128], P('group'), parts along dimension 0
The draws below stay inside these ranges and needn't reach their ends.
There are 4 independent parts, one for each index of `group`. The reference program is written for one: setup_inputs(seed, part) draws one part's arguments, and reference() takes and returns one part's arrays. A program takes and returns all parts, laid end to end along the dimension named above; each array names one. Nothing has to cross between parts.
All inputs are finite; a program needn't handle non-finite values. No bound on the sum of `flags` on one device may be relied on, other than what follows from the above.
Results may differ from the reference program's by a relative error of at most 0.004.
Values may be sent and summed in bfloat16 or wider, within the bound.
No kernel may reach another device: no remote copies, remote signals or barrier semaphores. Data moves between devices by JAX's collectives and lax.ppermute only.
A program may use at most 192 MiB of HBM per device.

```python
import math
import jax
import jax.numpy as jnp
from jax import lax

NF = 1024
NT = 16
CB = 128
BW = 32
BL = 512
NCB = 8


def taper_curve():
    angle = jnp.arange(NF, dtype=jnp.int32).astype(jnp.float32) * (2.0 * math.pi / (NF - 1))
    return 0.35875 - 0.48829 * jnp.cos(angle) + 0.14128 * jnp.cos(2.0 * angle) - 0.01168 * jnp.cos(3.0 * angle)


def draw_visibilities(key, part):
    noise_key = jax.random.fold_in(key, 11)
    shape = (2, BL, NT, NF)
    floor_level = 0.01
    noise = jax.random.truncated_normal(noise_key, -6.0, 6.0, shape, jnp.float32)
    envelope = 0.6 * (1.0 + floor_level) / (taper_curve() + floor_level)
    return (noise * envelope[None, None, None, :]).astype(jnp.float32)


def plant(values, rng, smallest, high):
    extent = values.shape
    place = [jax.random.randint(jax.random.fold_in(rng, axis), (), 0, extent[axis]) for axis in range(len(extent))]
    values = values.at[tuple(place)].set(smallest)
    longest = extent.index(max(extent))
    place[longest] = (place[longest] + 1) % extent[longest]
    return values.at[tuple(place)].set(high)


def setup_inputs(seed: int = 0, part: int = 0) -> dict:
    key_list = jax.random.split(jax.random.key(seed), 3)
    part_keys = jax.random.split(jax.random.fold_in(key_list[2], part), 3)
    visibilities = draw_visibilities(jax.random.fold_in(jax.random.fold_in(key_list[2], part), 71), part)
    flags = plant((jax.random.randint(part_keys[1], (BL, NCB), 0, 8) < 7).astype(jnp.int32), jax.random.fold_in(part_keys[1], 1), 0, 1)
    return dict(visibilities=visibilities, flags=flags)


def make_taper():
    angle = jnp.arange(NF, dtype=jnp.int32).astype(jnp.float32) * (2.0 * math.pi / (NF - 1))
    return 0.35875 - 0.48829 * jnp.cos(angle) + 0.14128 * jnp.cos(2.0 * angle) - 0.01168 * jnp.cos(3.0 * angle)

def make_tables():
    index = jnp.arange(NF, dtype=jnp.int32)
    phase = index[:, None] * index[None, :] % NF
    angle = phase.astype(jnp.float32) * (2.0 * math.pi / NF)
    return (jnp.cos(angle), jnp.sin(angle))

def delay_spectra(visibilities, flags):
    count = visibilities.shape[1]
    keep = jnp.broadcast_to(flags[:, :, None], (count, NF // CB, CB)).reshape(count, NF).astype(jnp.float32)
    weight = keep * make_taper()[None, :]
    tapered = visibilities * weight[None, :, None, :]
    real_rows = tapered[0].reshape(count * NT, NF)
    imag_rows = tapered[1].reshape(count * NT, NF)
    cosine, sine = make_tables()
    high = lax.Precision.HIGHEST
    scale = 1.0 / math.sqrt(NF)
    real_out = (jnp.dot(real_rows, cosine, precision=high) + jnp.dot(imag_rows, sine, precision=high)) * scale
    imag_out = (jnp.dot(imag_rows, cosine, precision=high) - jnp.dot(real_rows, sine, precision=high)) * scale
    stacked = jnp.stack([real_out.reshape(count, NT, NF), imag_out.reshape(count, NT, NF)], 2)
    stacked = stacked.reshape(count, NT, 2, NF // BW, BW).transpose(3, 0, 1, 2, 4)
    return stacked.reshape(NF // BW, count, NT * 2 * BW).astype(jnp.bfloat16)

def reference(visibilities, flags):
    delayed = delay_spectra(visibilities, flags).astype(jnp.float32)
    cross_power = jnp.einsum('kbj,kcj->kbc', delayed, delayed, precision=lax.Precision.HIGHEST) / NT
    self_power = lax.optimization_barrier(jnp.sum(delayed * delayed, axis=2)) / NT
    bandpower = (lax.optimization_barrier(jnp.sum(cross_power, axis=(1, 2))) - lax.optimization_barrier(jnp.sum(self_power, axis=1))) / visibilities.shape[1]
    return (cross_power, bandpower)
```

```python
import math

import jax
import jax.numpy as jnp
import numpy as np
from jax import lax
from jax.experimental import pallas as pl
from jax.experimental.pallas import tpu as pltpu
from jax.sharding import PartitionSpec as P

NF = 1024
NT = 16
CB = 128
BW = 32
NCB = 8
NB = NF // BW
HALF_ROOT = math.sqrt(0.5)


def taper_table():
    angle = np.arange(NF, dtype=np.float64) * (2.0 * math.pi / (NF - 1))
    taper = 0.35875 - 0.48829 * np.cos(angle) + 0.14128 * np.cos(2.0 * angle) - 0.01168 * np.cos(3.0 * angle)
    return jnp.asarray(taper.astype(np.float32).reshape(NCB, CB))


def transform_tables():
    r = np.arange(8)[:, None, None]
    h = np.arange(128)[None, :, None]
    g = np.arange(CB)[None, None, :]
    phi = ((8 * h + r) * g % NF) * (2.0 * math.pi / NF)
    scale = 1.0 / math.sqrt(NF)
    cosine, sine = np.cos(phi) * scale, np.sin(phi) * scale
    real = np.concatenate([cosine, sine], 2).reshape(8, NB, 1, 4, 2 * CB)
    imag = np.concatenate([-sine, cosine], 2).reshape(8, NB, 1, 4, 2 * CB)
    full = np.concatenate([real, imag], 2).reshape(8, 2 * CB, 2 * CB)
    high = full.astype(jnp.bfloat16)
    low = (full - high.astype(np.float64)).astype(jnp.bfloat16)
    return jnp.asarray(high), jnp.asarray(low)


def fold8(re, im):
    def two(a, b):
        return (a[0] + b[0], a[1] + b[1]), (a[0] - b[0], a[1] - b[1])

    def turn(a):
        return (a[1], -a[0])

    def four(x0, x1, x2, x3):
        s0, d0 = two(x0, x2)
        s1, d1 = two(x1, x3)
        y0, y2 = two(s0, s1)
        d1 = turn(d1)
        y1, y3 = two(d0, d1)
        return y0, y1, y2, y3

    x = list(zip(re, im))
    even = four(x[0], x[2], x[4], x[6])
    odd = four(x[1], x[3], x[5], x[7])
    o1 = odd[1]
    o3 = odd[3]
    w1 = ((o1[0] + o1[1]) * HALF_ROOT, (o1[1] - o1[0]) * HALF_ROOT)
    w3 = ((o3[1] - o3[0]) * HALF_ROOT, -(o3[0] + o3[1]) * HALF_ROOT)
    out = [None] * 8
    for i, o in enumerate((odd[0], w1, turn(odd[2]), w3)):
        out[i], out[i + 4] = two(even[i], o)
    return out


def spectra_kernel(x_hbm, flags_ref, taper_ref, high_ref, low_ref, out_ref, xs, yh, yl, z, sems):
    copies = [
        pltpu.make_async_copy(x_hbm.at[part, :, t, :], xs.at[part, t], sems.at[part, t])
        for t in range(NT)
        for part in range(2)
    ]
    for c in copies:
        c.start()
    rows = flags_ref.shape[0]
    weight = []
    for a in range(NCB):
        keep = jnp.broadcast_to(flags_ref[:, a : a + 1].astype(jnp.float32), (rows, CB))
        weight.append(keep * taper_ref[a : a + 1, :])
    for t in range(NT):
        copies[2 * t].wait()
        copies[2 * t + 1].wait()
        parts = [[xs[part, t, :, a * CB : (a + 1) * CB] * weight[a] for a in range(NCB)] for part in range(2)]
        folded = fold8(*parts)
        for r in range(8):
            for part in range(2):
                value = folded[r][part]
                high = value.astype(jnp.bfloat16)
                yh[r, t * rows : (t + 1) * rows, part * CB : (part + 1) * CB] = high
                yl[r, t * rows : (t + 1) * rows, part * CB : (part + 1) * CB] = (
                    value - high.astype(jnp.float32)
                ).astype(jnp.bfloat16)
    dims = (((1,), (1,)), ((), ()))
    for r in range(8):
        z[r] = (
            lax.dot_general(high_ref[r], yh[r], dims, preferred_element_type=jnp.float32)
            + lax.dot_general(low_ref[r], yh[r], dims, preferred_element_type=jnp.float32)
            + lax.dot_general(high_ref[r], yl[r], dims, preferred_element_type=jnp.float32)
        )
    for k in range(NB):
        lower = z[:, 8 * k : 8 * k + 8, 0:128].reshape(64, 128)
        upper = z[:, 8 * k : 8 * k + 8, 128:256].reshape(64, 128)
        block = jnp.concatenate([lower, upper], 0).T.astype(jnp.bfloat16)
        for i in range(8):
            out_ref[k, :, i * 128 : (i + 1) * 128] = block[i * rows : (i + 1) * rows, :]


def spectra(visibilities, flags):
    rows = visibilities.shape[1]
    high, low = transform_tables()
    vmem = pl.BlockSpec(memory_space=pltpu.VMEM)
    return pl.pallas_call(
        spectra_kernel,
        out_shape=jax.ShapeDtypeStruct((NB, rows, NT * 2 * BW), jnp.bfloat16),
        in_specs=[pl.BlockSpec(memory_space=pl.ANY), vmem, vmem, vmem, vmem],
        out_specs=vmem,
        scratch_shapes=[
            pltpu.VMEM((2, NT, rows, NF), jnp.float32),
            pltpu.VMEM((8, NT * rows, 2 * CB), jnp.bfloat16),
            pltpu.VMEM((8, NT * rows, 2 * CB), jnp.bfloat16),
            pltpu.VMEM((8, 2 * CB, NT * rows), jnp.float32),
            pltpu.SemaphoreType.DMA((2, NT)),
        ],
        name="spectra",
    )(visibilities, flags, taper_table(), high, low)


def cross_kernel(own_ref, out_ref):
    count = out_ref.shape[0]
    rows = out_ref.shape[1]
    total = count * rows
    delayed = own_ref[...].reshape(total, own_ref.shape[2])
    power = lax.dot_general(
        delayed, delayed, (((1,), (1,)), ((), ())), preferred_element_type=jnp.float32
    ) * (1.0 / NT)
    out_ref[:, :, 0:total] = power.astype(jnp.bfloat16).reshape(count, rows, total)
    row = lax.broadcasted_iota(jnp.int32, (total, total), 0)
    col = lax.broadcasted_iota(jnp.int32, (total, total), 1)
    off = jnp.where(row == col, 0.0, power)
    band = jnp.sum(jnp.sum(off, axis=0, keepdims=True), axis=1, keepdims=True) * (1.0 / total)
    band = jnp.broadcast_to(band, (rows, 128))
    first = band.astype(jnp.bfloat16).astype(jnp.float32)
    second = (band - first).astype(jnp.bfloat16).astype(jnp.float32)
    third = band - first - second
    lane = lax.broadcasted_iota(jnp.int32, (rows, 128), 1)
    tail = jnp.where(lane == 0, first, jnp.where(lane == 1, second, jnp.where(lane == 2, third, 0.0)))
    tail = tail.astype(jnp.bfloat16)
    for s in range(count):
        out_ref[s, :, total : total + 128] = tail


def cross(delayed):
    count, rows, _ = delayed.shape
    vmem = pl.BlockSpec(memory_space=pltpu.VMEM)
    return pl.pallas_call(
        cross_kernel,
        out_shape=jax.ShapeDtypeStruct((count, rows, count * rows + 128), jnp.bfloat16),
        in_specs=[vmem],
        out_specs=vmem,
        name="cross",
    )(delayed)


def shards(visibilities, flags):
    own = spectra(visibilities, flags)
    mine = lax.all_to_all(own, "bl", 0, 0, tiled=True)
    back = lax.all_to_all(cross(mine), "bl", 0, 0, tiled=True)
    total = back.shape[2] - 128
    power = back[:, :, :total].astype(jnp.float32)
    band = jnp.sum(back[:, 0, total : total + 3].astype(jnp.float32), axis=1)
    return (power, band)


def solution(mesh):
    return jax.shard_map(
        shards,
        mesh=mesh,
        in_specs=(P(None, ("group", "bl"), None, None), P(("group", "bl"), None)),
        out_specs=(P(None, ("group", "bl"), None), P("group")),
        check_vma=False,
    )
```

```python
import math

import jax
import jax.numpy as jnp
import numpy as np
from jax import lax
from jax.experimental import pallas as pl
from jax.experimental.pallas import tpu as pltpu
from jax.sharding import PartitionSpec as P

NF = 1024
NT = 16
CB = 128
BW = 32
NCB = 8
NB = NF // BW
HALF_ROOT = math.sqrt(0.5)


def taper_table():
    angle = np.arange(NF, dtype=np.float64) * (2.0 * math.pi / (NF - 1))
    taper = 0.35875 - 0.48829 * np.cos(angle) + 0.14128 * np.cos(2.0 * angle) - 0.01168 * np.cos(3.0 * angle)
    return jnp.asarray(taper.astype(np.float32).reshape(NCB, CB))


def transform_tables():
    r = np.arange(8)[:, None, None]
    h = np.arange(128)[None, :, None]
    g = np.arange(CB)[None, None, :]
    phi = ((8 * h + r) * g % NF) * (2.0 * math.pi / NF)
    scale = 1.0 / math.sqrt(NF)
    cosine, sine = np.cos(phi) * scale, np.sin(phi) * scale
    real = np.concatenate([cosine, sine], 2).reshape(8, NB, 1, 4, 2 * CB)
    imag = np.concatenate([-sine, cosine], 2).reshape(8, NB, 1, 4, 2 * CB)
    full = np.concatenate([real, imag], 2).reshape(8, 2 * CB, 2 * CB)
    high = full.astype(jnp.bfloat16)
    low = (full - high.astype(np.float64)).astype(jnp.bfloat16)
    return jnp.asarray(high), jnp.asarray(low)


def fold8(re, im):
    def two(a, b):
        return (a[0] + b[0], a[1] + b[1]), (a[0] - b[0], a[1] - b[1])

    def turn(a):
        return (a[1], -a[0])

    def four(x0, x1, x2, x3):
        s0, d0 = two(x0, x2)
        s1, d1 = two(x1, x3)
        y0, y2 = two(s0, s1)
        d1 = turn(d1)
        y1, y3 = two(d0, d1)
        return y0, y1, y2, y3

    x = list(zip(re, im))
    even = four(x[0], x[2], x[4], x[6])
    odd = four(x[1], x[3], x[5], x[7])
    o1 = odd[1]
    o3 = odd[3]
    w1 = ((o1[0] + o1[1]) * HALF_ROOT, (o1[1] - o1[0]) * HALF_ROOT)
    w3 = ((o3[1] - o3[0]) * HALF_ROOT, -(o3[0] + o3[1]) * HALF_ROOT)
    out = [None] * 8
    for i, o in enumerate((odd[0], w1, turn(odd[2]), w3)):
        out[i], out[i + 4] = two(even[i], o)
    return out


def spectra_kernel(x_hbm, flags_ref, taper_ref, high_hbm, low_hbm, out_hbm, xs, yh, yl, z, high_ref, low_ref, out_ref, sems, table_sems, out_sems):
    copies = [
        pltpu.make_async_copy(x_hbm.at[part, :, t, :], xs.at[part, t], sems.at[part, t])
        for t in range(NT)
        for part in range(2)
    ]
    for c in copies:
        c.start()
    tables = [
        pltpu.make_async_copy(high_hbm, high_ref, table_sems.at[0]),
        pltpu.make_async_copy(low_hbm, low_ref, table_sems.at[1]),
    ]
    for c in tables:
        c.start()
    rows = flags_ref.shape[1]
    flags = flags_ref[...].astype(jnp.float32).T
    weight = []
    for a in range(NCB):
        keep = jnp.broadcast_to(flags[:, a : a + 1], (rows, CB))
        weight.append(keep * taper_ref[a : a + 1, :])
    for t in range(NT):
        copies[2 * t].wait()
        copies[2 * t + 1].wait()
        parts = [[xs[part, t, :, a * CB : (a + 1) * CB] * weight[a] for a in range(NCB)] for part in range(2)]
        folded = fold8(*parts)
        for r in range(8):
            for part in range(2):
                value = folded[r][part]
                high = value.astype(jnp.bfloat16)
                yh[r, t * rows : (t + 1) * rows, part * CB : (part + 1) * CB] = high
                yl[r, t * rows : (t + 1) * rows, part * CB : (part + 1) * CB] = (
                    value - high.astype(jnp.float32)
                ).astype(jnp.bfloat16)
    for c in tables:
        c.wait()
    dims = (((1,), (1,)), ((), ()))
    for r in range(8):
        z[r] = (
            lax.dot_general(high_ref[r], yh[r], dims, preferred_element_type=jnp.float32)
            + lax.dot_general(low_ref[r], yh[r], dims, preferred_element_type=jnp.float32)
            + lax.dot_general(high_ref[r], yl[r], dims, preferred_element_type=jnp.float32)
        )
    sends = []
    for k in range(NB):
        lower = z[:, 8 * k : 8 * k + 8, 0:128].reshape(64, 128)
        upper = z[:, 8 * k : 8 * k + 8, 128:256].reshape(64, 128)
        block = jnp.concatenate([lower, upper], 0).T.astype(jnp.bfloat16)
        for i in range(8):
            out_ref[k, :, i * 128 : (i + 1) * 128] = block[i * rows : (i + 1) * rows, :]
        if k % 8 == 7:
            part = pl.ds(k - 7, 8)
            sends.append(pltpu.make_async_copy(out_ref.at[part], out_hbm.at[part], out_sems.at[k // 8]))
            sends[-1].start()
    for c in sends:
        c.wait()


def spectra(visibilities, flags):
    rows = visibilities.shape[1]
    high, low = transform_tables()
    vmem = pl.BlockSpec(memory_space=pltpu.VMEM)
    hbm = pl.BlockSpec(memory_space=pltpu.HBM)
    return pl.pallas_call(
        spectra_kernel,
        out_shape=jax.ShapeDtypeStruct((NB, rows, NT * 2 * BW), jnp.bfloat16),
        in_specs=[hbm, vmem, vmem, hbm, hbm],
        out_specs=hbm,
        compiler_params=pltpu.CompilerParams(vmem_limit_bytes=63 << 20),
        scratch_shapes=[
            pltpu.VMEM((2, NT, rows, NF), jnp.float32),
            pltpu.VMEM((8, NT * rows, 2 * CB), jnp.bfloat16),
            pltpu.VMEM((8, NT * rows, 2 * CB), jnp.bfloat16),
            pltpu.VMEM((8, 2 * CB, NT * rows), jnp.float32),
            pltpu.VMEM(high.shape, jnp.bfloat16),
            pltpu.VMEM(low.shape, jnp.bfloat16),
            pltpu.VMEM((NB, rows, NT * 2 * BW), jnp.bfloat16),
            pltpu.SemaphoreType.DMA((2, NT)),
            pltpu.SemaphoreType.DMA((2,)),
            pltpu.SemaphoreType.DMA((NB // 8,)),
        ],
        name="spectra",
    )(visibilities, flags.T, taper_table(), high, low)


def cross_kernel(own_ref, out_ref):
    count, rows, _ = out_ref.shape
    total = count * rows
    delayed = own_ref[...].reshape(total, own_ref.shape[2])
    power = lax.dot_general(
        delayed, delayed, (((1,), (1,)), ((), ())), preferred_element_type=jnp.float32
    ) * (1.0 / NT)
    out_ref[:, :, 0:total] = power.astype(jnp.bfloat16).reshape(count, rows, total)
    row = lax.broadcasted_iota(jnp.int32, (total, total), 0)
    col = lax.broadcasted_iota(jnp.int32, (total, total), 1)
    off = jnp.where(row == col, 0.0, power)
    band = jnp.sum(jnp.sum(off, axis=0, keepdims=True), axis=1, keepdims=True) * (1.0 / total)
    band = jnp.broadcast_to(band, (rows, total))
    first = band.astype(jnp.bfloat16).astype(jnp.float32)
    second = (band - first).astype(jnp.bfloat16).astype(jnp.float32)
    third = band - first - second
    row = lax.broadcasted_iota(jnp.int32, (rows, total), 0)
    col = lax.broadcasted_iota(jnp.int32, (rows, total), 1)
    term = jnp.where(row == 1, first, jnp.where(row == 2, second, third))
    spare = (row >= 1) & (row <= 3)
    for s in range(count):
        piece = power[s * rows : (s + 1) * rows]
        out_ref[s] = jnp.where(spare & (col == s * rows), term, piece).astype(jnp.bfloat16)


def cross(delayed):
    count, rows, _ = delayed.shape
    vmem = pl.BlockSpec(memory_space=pltpu.VMEM)
    return pl.pallas_call(
        cross_kernel,
        out_shape=jax.ShapeDtypeStruct((count, rows, count * rows), jnp.bfloat16),
        in_specs=[vmem],
        out_specs=vmem,
        compiler_params=pltpu.CompilerParams(vmem_limit_bytes=8 << 20),
        name="cross",
    )(delayed)


def finish_kernel(back_ref, power_ref, band_ref):
    bands, rows, total = back_ref.shape
    start = lax.axis_index("bl") * rows
    power = back_ref[...].astype(jnp.float32)
    power_ref[...] = power
    lane = lax.broadcasted_iota(jnp.int32, (bands, total), 1)
    top = power[:, 0, :]
    band = jnp.zeros((bands, 1), jnp.float32)
    for i in range(1, 4):
        line = power[:, i, :]
        band += jnp.sum(jnp.where(lane == start, line, 0.0), axis=1, keepdims=True)
        value = jnp.sum(jnp.where(lane == start + i, top, 0.0), axis=1, keepdims=True)
        power_ref[:, i, :] = jnp.where(lane == start, value, line)
    row = lax.broadcasted_iota(jnp.int32, (bands, bands), 0)
    col = lax.broadcasted_iota(jnp.int32, (bands, bands), 1)
    band_ref[...] = jnp.sum(jnp.where(row == col, band, 0.0), axis=0, keepdims=True)


def finish(back):
    bands, rows, total = back.shape
    vmem = pl.BlockSpec(memory_space=pltpu.VMEM)
    return pl.pallas_call(
        finish_kernel,
        out_shape=(
            jax.ShapeDtypeStruct((bands, rows, total), jnp.float32),
            jax.ShapeDtypeStruct((1, bands), jnp.float32),
        ),
        in_specs=[vmem],
        out_specs=(vmem, vmem),
        compiler_params=pltpu.CompilerParams(vmem_limit_bytes=8 << 20),
        name="finish",
    )(back)


def shards(visibilities, flags):
    own = spectra(visibilities, flags)
    mine = lax.all_to_all(own, "bl", 0, 0, tiled=True)
    back = lax.all_to_all(cross(mine), "bl", 0, 0, tiled=True)
    power, band = finish(back)
    return (power, band.reshape(-1))


def solution(mesh):
    return jax.shard_map(
        shards,
        mesh=mesh,
        in_specs=(P(None, ("group", "bl"), None, None), P(("group", "bl"), None)),
        out_specs=(P(None, ("group", "bl"), None), P("group")),
        check_vma=False,
    )
```

```python
import math

import jax
import jax.numpy as jnp
import numpy as np
from jax import lax
from jax.experimental import pallas as pl
from jax.experimental.pallas import tpu as pltpu
from jax.sharding import PartitionSpec as P

NF = 1024
NT = 16
CB = 128
BW = 32
NCB = 8
NB = NF // BW
HALF_ROOT = math.sqrt(0.5)


def taper_table():
    angle = np.arange(NF, dtype=np.float64) * (2.0 * math.pi / (NF - 1))
    taper = 0.35875 - 0.48829 * np.cos(angle) + 0.14128 * np.cos(2.0 * angle) - 0.01168 * np.cos(3.0 * angle)
    return jnp.asarray(taper.astype(np.float32).reshape(NCB, CB))


def transform_tables():
    r = np.arange(5)[:, None, None]
    h = np.arange(128)[None, :, None]
    g = np.arange(CB)[None, None, :]
    phi = ((8 * h + r) * g % NF) * (2.0 * math.pi / NF)
    scale = 1.0 / math.sqrt(NF)
    cosine, sine = np.cos(phi) * scale, np.sin(phi) * scale
    real = np.concatenate([cosine, sine], 2).reshape(5, NB, 1, 4, 2 * CB)
    imag = np.concatenate([-sine, cosine], 2).reshape(5, NB, 1, 4, 2 * CB)
    full = np.concatenate([real, imag], 2).reshape(5, 2 * CB, 2 * CB)
    high = full.astype(jnp.bfloat16)
    low = (full - high.astype(np.float64)).astype(jnp.bfloat16)
    return jnp.asarray(np.stack([high, low], 1))


def two(a, b):
    return (a[0] + b[0], a[1] + b[1]), (a[0] - b[0], a[1] - b[1])


def four(x0, x1, x2, x3, conjugated):
    s0, d0 = two(x0, x2)
    s1, d1 = two(x1, x3)
    d1 = (d1[1], -d1[0])
    y = [*two(s0, s1), *two(d0, d1)]
    y = [y[0], y[2], y[1], y[3]]
    minus = {2: (s1, s0), 3: (d1, d0)}
    for i in conjugated:
        y[i] = (y[i][0], minus[i][0][1] - minus[i][1][1])
    return y


def split_store(value, high_ref, low_ref, r, row, part):
    high = value.astype(jnp.bfloat16)
    at = (r, pl.ds(row, value.shape[0]), pl.ds(part * CB, CB))
    high_ref[at] = high
    low_ref[at] = (value - high.astype(jnp.float32)).astype(jnp.bfloat16)


def spectra_kernel(
    x_hbm, flags_hbm, taper_hbm, table_hbm, out_ref, xs, flags_ref, taper_ref, yh, yl, z, table, sems, side_sems
):
    rows = flags_ref.shape[1]
    small = [
        pltpu.make_async_copy(flags_hbm, flags_ref, side_sems.at[0]),
        pltpu.make_async_copy(taper_hbm, taper_ref, side_sems.at[1]),
    ]
    copies = [
        pltpu.make_async_copy(x_hbm.at[part, :, t, :], xs.at[part, t], sems.at[part, t])
        for t in range(NT)
        for part in range(2)
    ]
    tables = pltpu.make_async_copy(table_hbm, table, side_sems.at[2])
    for c in [*small, tables, *copies]:
        c.start()
    for c in small:
        c.wait()
    flags = flags_ref[...].astype(jnp.float32).T
    weight = []
    for a in range(NCB):
        keep = jnp.broadcast_to(flags[:, a : a + 1], (rows, CB))
        weight.append(keep * taper_ref[a : a + 1, :])

    def lanes(a):
        return slice(a * CB, (a + 1) * CB)

    def multiply(r):
        dims = (((1,), (1,)), ((), ()))
        i = min(r, 8 - r)
        z[r] = (
            lax.dot_general(table[i, 0], yh[r], dims, preferred_element_type=jnp.float32)
            + lax.dot_general(table[i, 1], yh[r], dims, preferred_element_type=jnp.float32)
            + lax.dot_general(table[i, 0], yl[r], dims, preferred_element_type=jnp.float32)
        )

    for t in range(NT):
        copies[2 * t].wait()
        copies[2 * t + 1].wait()
        u = [tuple(xs[part, t, :, lanes(a)] * weight[a] for part in range(2)) for a in range(NCB)]
        pairs = [two(u[a], u[a + 4]) for a in range(4)]
        for a in range(4):
            for part in range(2):
                xs[part, t, :, lanes(a)] = pairs[a][1][part]
        y = four(*(p[0] for p in pairs), conjugated=(3,))
        for m in range(4):
            for part in range(2):
                split_store(y[m][part], yh, yl, 2 * m, t * rows, part)
    tables.wait()
    for t in range(NT):
        if t % 4 == 0:
            multiply((0, 4, 2, 6)[t // 4])
        d = [tuple(xs[part, t, :, lanes(a)] for part in range(2)) for a in range(4)]
        d[1] = ((d[1][0] + d[1][1]) * HALF_ROOT, (d[1][1] - d[1][0]) * HALF_ROOT)
        d[2] = (d[2][1], -d[2][0])
        d[3] = ((d[3][1] - d[3][0]) * HALF_ROOT, (d[3][0] + d[3][1]) * -HALF_ROOT)
        y = four(*d, conjugated=(2, 3))
        for m in range(4):
            for part in range(2):
                split_store(y[m][part], yh, yl, 2 * m + 1, t * rows, part)
    for r in (1, 7, 3, 5):
        multiply(r)
    for k in range(NB):
        straight, turned = pl.ds(8 * k, 8), pl.ds(8 * (NB - 1 - k), 8)
        lower = jnp.concatenate([z[r, straight if r < 5 else turned, 0:128] for r in range(8)], 0)
        upper = jnp.concatenate([z[r, straight if r < 5 else turned, 128:256] for r in range(8)], 0)
        block = jnp.concatenate([lower, upper], 0).T.astype(jnp.bfloat16)
        for i in range(8):
            out_ref[k, :, i * 128 : (i + 1) * 128] = block[i * rows : (i + 1) * rows, :]


def in_hbm(array):
    return pltpu.with_memory_space_constraint(array, pltpu.HBM)


def spectra(visibilities, flags):
    rows = visibilities.shape[1]
    table = transform_tables()
    hbm = pl.BlockSpec(memory_space=pltpu.HBM)
    return pl.pallas_call(
        spectra_kernel,
        out_shape=pltpu.VMEM((NB, rows, NT * 2 * BW), jnp.bfloat16),
        in_specs=[hbm] * 4,
        out_specs=pl.BlockSpec(memory_space=pltpu.VMEM),
        compiler_params=pltpu.CompilerParams(vmem_limit_bytes=24 << 20),
        scratch_shapes=[
            pltpu.VMEM((2, NT, rows, NF), jnp.float32),
            pltpu.VMEM((NCB, rows), jnp.int32),
            pltpu.VMEM((NCB, CB), jnp.float32),
            pltpu.VMEM((8, NT * rows, 2 * CB), jnp.bfloat16),
            pltpu.VMEM((8, NT * rows, 2 * CB), jnp.bfloat16),
            pltpu.VMEM((8, 2 * CB, NT * rows), jnp.float32),
            pltpu.VMEM(table.shape, jnp.bfloat16),
            pltpu.SemaphoreType.DMA((2, NT)),
            pltpu.SemaphoreType.DMA((3,)),
        ],
        name="spectra",
    )(in_hbm(visibilities), in_hbm(flags.T), in_hbm(taper_table()), in_hbm(table))


def cross_kernel(own_ref, out_ref):
    count, rows, _ = out_ref.shape
    total = count * rows
    delayed = own_ref[...].reshape(total, own_ref.shape[2])
    power = lax.dot_general(
        delayed, delayed, (((1,), (1,)), ((), ())), preferred_element_type=jnp.float32
    ) * (1.0 / NT)
    out_ref[:, :, 0:total] = power.astype(jnp.bfloat16).reshape(count, rows, total)
    row = lax.broadcasted_iota(jnp.int32, (total, total), 0)
    col = lax.broadcasted_iota(jnp.int32, (total, total), 1)
    off = jnp.where(row == col, 0.0, power)
    band = jnp.sum(jnp.sum(off, axis=0, keepdims=True), axis=1, keepdims=True) * (1.0 / total)
    band = jnp.broadcast_to(band, (rows, total))
    first = band.astype(jnp.bfloat16).astype(jnp.float32)
    second = (band - first).astype(jnp.bfloat16).astype(jnp.float32)
    third = band - first - second
    row = lax.broadcasted_iota(jnp.int32, (rows, total), 0)
    col = lax.broadcasted_iota(jnp.int32, (rows, total), 1)
    term = jnp.where(row == 1, first, jnp.where(row == 2, second, third))
    spare = (row >= 1) & (row <= 3)
    for s in range(count):
        piece = power[s * rows : (s + 1) * rows]
        out_ref[s] = jnp.where(spare & (col == s * rows), term, piece).astype(jnp.bfloat16)


def cross(delayed):
    count, rows, _ = delayed.shape
    vmem = pl.BlockSpec(memory_space=pltpu.VMEM)
    return pl.pallas_call(
        cross_kernel,
        out_shape=jax.ShapeDtypeStruct((count, rows, count * rows), jnp.bfloat16),
        in_specs=[vmem],
        out_specs=vmem,
        compiler_params=pltpu.CompilerParams(vmem_limit_bytes=8 << 20),
        name="cross",
    )(delayed)


def finish_kernel(back_ref, power_ref, band_ref):
    bands, rows, total = back_ref.shape
    start = lax.axis_index("bl") * rows
    power = back_ref[...].astype(jnp.float32)
    power_ref[...] = power
    lane = lax.broadcasted_iota(jnp.int32, (bands, total), 1)
    top = power[:, 0, :]
    band = jnp.zeros((bands, 1), jnp.float32)
    for i in range(1, 4):
        line = power[:, i, :]
        band += jnp.sum(jnp.where(lane == start, line, 0.0), axis=1, keepdims=True)
        value = jnp.sum(jnp.where(lane == start + i, top, 0.0), axis=1, keepdims=True)
        power_ref[:, i, :] = jnp.where(lane == start, value, line)
    row = lax.broadcasted_iota(jnp.int32, (bands, bands), 0)
    col = lax.broadcasted_iota(jnp.int32, (bands, bands), 1)
    band_ref[...] = jnp.sum(jnp.where(row == col, band, 0.0), axis=0, keepdims=True)


def finish(back):
    bands, rows, total = back.shape
    vmem = pl.BlockSpec(memory_space=pltpu.VMEM)
    return pl.pallas_call(
        finish_kernel,
        out_shape=(
            jax.ShapeDtypeStruct((bands, rows, total), jnp.float32),
            jax.ShapeDtypeStruct((1, bands), jnp.float32),
        ),
        in_specs=[vmem],
        out_specs=(vmem, vmem),
        compiler_params=pltpu.CompilerParams(vmem_limit_bytes=8 << 20),
        name="finish",
    )(back)


def shards(visibilities, flags):
    own = spectra(visibilities, flags)
    mine = lax.all_to_all(own, "bl", 0, 0, tiled=True)
    back = lax.all_to_all(cross(mine), "bl", 0, 0, tiled=True)
    power, band = finish(back)
    return (power, band.reshape(-1))


def solution(mesh):
    return jax.shard_map(
        shards,
        mesh=mesh,
        in_specs=(P(None, ("group", "bl"), None, None), P(("group", "bl"), None)),
        out_specs=(P(None, ("group", "bl"), None), P("group")),
        check_vma=False,
    )
```

```python
import math

import jax
import jax.numpy as jnp
import numpy as np
from jax import lax
from jax.experimental import pallas as pl
from jax.experimental.pallas import tpu as pltpu
from jax.sharding import PartitionSpec as P

NF = 1024
NT = 16
CB = 128
BW = 32
NCB = 8
NB = NF // BW
GROUP = 4
HALF_ROOT = math.sqrt(0.5)
OUT = [(-3 * i % 32) ^ 26 for i in range(32)]
BACK = [(-3 * i % 32) ^ 26 for i in range(32)]


def taper_table():
    angle = np.arange(NF, dtype=np.float64) * (2.0 * math.pi / (NF - 1))
    taper = 0.35875 - 0.48829 * np.cos(angle) + 0.14128 * np.cos(2.0 * angle) - 0.01168 * np.cos(3.0 * angle)
    return taper.reshape(NCB, CB)


def transform_table():
    h = np.arange(128)[:, None]
    g = np.arange(CB)[None, :]
    phi = (h * g % CB) * (2.0 * math.pi / CB)
    scale = 1.0 / math.sqrt(NF)
    cosine, sine = np.cos(phi) * scale, np.sin(phi) * scale
    real = np.concatenate([cosine, sine], 1).reshape(NB, 1, 4, 2 * CB)
    imag = np.concatenate([-sine, cosine], 1).reshape(NB, 1, 4, 2 * CB)
    full = np.concatenate([real, imag], 1).reshape(2 * CB, 2 * CB)
    high = full.astype(jnp.bfloat16)
    low = (full - high.astype(np.float64)).astype(jnp.bfloat16)
    return jnp.asarray(np.stack([high, low]))


def row_table():
    phi = np.arange(8)[:, None] * np.arange(CB)[None, :] * (2.0 * math.pi / NF)
    return jnp.asarray(np.concatenate([taper_table(), np.cos(phi), np.sin(phi)]).astype(np.float32))


def two(a, b):
    return (a[0] + b[0], a[1] + b[1]), (a[0] - b[0], a[1] - b[1])


def four(x0, x1, x2, x3):
    s0, d0 = two(x0, x2)
    s1, d1 = two(x1, x3)
    y0, y2 = two(s0, s1)
    y1, y3 = two(d0, (d1[1], -d1[0]))
    return y0, y1, y2, y3


def eight(x):
    pairs = [two(x[a], x[a + 4]) for a in range(4)]
    d = [p[1] for p in pairs]
    d[1] = ((d[1][0] + d[1][1]) * HALF_ROOT, (d[1][1] - d[1][0]) * HALF_ROOT)
    d[2] = (d[2][1], -d[2][0])
    d[3] = ((d[3][1] - d[3][0]) * HALF_ROOT, (d[3][0] + d[3][1]) * -HALF_ROOT)
    even, odd = four(*(p[0] for p in pairs)), four(*d)
    return [even[0], odd[0], even[1], odd[1], even[2], odd[2], even[3], odd[3]]


def spectra_kernel(x_hbm, flags_hbm, rows_hbm, table_hbm, out_ref, xs, flags_ref, rows_ref, yh, yl, z, table, sems, side_sems):
    rows = flags_ref.shape[1]
    small = [
        pltpu.make_async_copy(flags_hbm, flags_ref, side_sems.at[0]),
        pltpu.make_async_copy(rows_hbm, rows_ref, side_sems.at[1]),
    ]
    copies = [
        pltpu.make_async_copy(x_hbm.at[part, :, t, :], xs.at[part, t], sems.at[part, t])
        for t in range(NT)
        for part in range(2)
    ]
    tables = pltpu.make_async_copy(table_hbm, table, side_sems.at[2])
    for c in [*small, tables, *copies]:
        c.start()
    for c in small:
        c.wait()
    flags = flags_ref[...].astype(jnp.float32).T
    weight = []
    for a in range(NCB):
        keep = jnp.broadcast_to(flags[:, a : a + 1], (rows, CB))
        weight.append(keep * rows_ref[a : a + 1, :])

    def fold(t):
        u = [
            tuple(xs[part, t, :, a * CB : (a + 1) * CB] * weight[a] for part in range(2)) for a in range(NCB)
        ]
        y = eight(u)
        for r in range(8):
            re, im = y[r]
            if r:
                cosine, sine = rows_ref[8 + r : 9 + r, :], rows_ref[16 + r : 17 + r, :]
                re, im = re * cosine + im * sine, im * cosine - re * sine
            at = pl.ds((r * GROUP + t % GROUP) * rows, rows)
            for part, value in enumerate((re, im)):
                high = value.astype(jnp.bfloat16)
                yh[t // GROUP, at, part * CB : (part + 1) * CB] = high
                low = (value - high.astype(jnp.float32)).astype(jnp.bfloat16)
                yl[t // GROUP, at, part * CB : (part + 1) * CB] = low

    def multiply(g):
        width = yh.shape[1]
        dims = (((1,), (1,)), ((), ()))
        z[:, g * width : (g + 1) * width] = (
            lax.dot_general(table[0], yh[g], dims, preferred_element_type=jnp.float32)
            + lax.dot_general(table[1], yh[g], dims, preferred_element_type=jnp.float32)
            + lax.dot_general(table[0], yl[g], dims, preferred_element_type=jnp.float32)
        )

    for g in range(NT // GROUP):
        for c in copies[2 * GROUP * g : 2 * GROUP * (g + 1)]:
            c.wait()
        if g == 1:
            tables.wait()
        if g:
            multiply(g - 1)
        for t in range(g * GROUP, (g + 1) * GROUP):
            fold(t)
    multiply(NT // GROUP - 1)
    for k in range(NB):
        tiles = [z[8 * k : 8 * k + 8, m * 128 : (m + 1) * 128] for m in range(z.shape[1] // 128)]
        block = jnp.concatenate(tiles, 0).T.astype(jnp.bfloat16)
        for i in range(8):
            out_ref[k, :, i * 128 : (i + 1) * 128] = block[i * rows : (i + 1) * rows, :]


def in_hbm(array):
    return pltpu.with_memory_space_constraint(array, pltpu.HBM)


def spectra(visibilities, flags):
    rows = visibilities.shape[1]
    table, row = transform_table(), row_table()
    hbm = pl.BlockSpec(memory_space=pltpu.HBM)
    return pl.pallas_call(
        spectra_kernel,
        out_shape=pltpu.VMEM((NB, rows, NT * 2 * BW), jnp.bfloat16),
        in_specs=[hbm] * 4,
        out_specs=pl.BlockSpec(memory_space=pltpu.VMEM),
        compiler_params=pltpu.CompilerParams(vmem_limit_bytes=24 << 20),
        scratch_shapes=[
            pltpu.VMEM((2, NT, rows, NF), jnp.float32),
            pltpu.VMEM((NCB, rows), jnp.int32),
            pltpu.VMEM(row.shape, jnp.float32),
            pltpu.VMEM((NT // GROUP, 8 * GROUP * rows, 2 * CB), jnp.bfloat16),
            pltpu.VMEM((NT // GROUP, 8 * GROUP * rows, 2 * CB), jnp.bfloat16),
            pltpu.VMEM((2 * CB, 8 * NT * rows), jnp.float32),
            pltpu.VMEM(table.shape, jnp.bfloat16),
            pltpu.SemaphoreType.DMA((2, NT)),
            pltpu.SemaphoreType.DMA((3,)),
        ],
        name="spectra",
    )(in_hbm(visibilities), in_hbm(flags.T), in_hbm(row), in_hbm(table))


def cross_kernel(own_ref, out_ref):
    count, rows, _ = out_ref.shape
    total = count * rows
    delayed = jnp.concatenate([own_ref[OUT.index(s)] for s in range(count)], 0)
    power = lax.dot_general(
        delayed, delayed, (((1,), (1,)), ((), ())), preferred_element_type=jnp.float32
    ) * (1.0 / NT)
    out_ref[:, :, 0:total] = power.astype(jnp.bfloat16).reshape(count, rows, total)
    row = lax.broadcasted_iota(jnp.int32, (total, total), 0)
    col = lax.broadcasted_iota(jnp.int32, (total, total), 1)
    off = jnp.where(row == col, 0.0, power)
    band = jnp.sum(jnp.sum(off, axis=0, keepdims=True), axis=1, keepdims=True) * (1.0 / total)
    band = jnp.broadcast_to(band, (rows, total))
    first = band.astype(jnp.bfloat16).astype(jnp.float32)
    second = (band - first).astype(jnp.bfloat16).astype(jnp.float32)
    third = band - first - second
    row = lax.broadcasted_iota(jnp.int32, (rows, total), 0)
    col = lax.broadcasted_iota(jnp.int32, (rows, total), 1)
    term = jnp.where(row == 1, first, jnp.where(row == 2, second, third))
    spare = (row >= 1) & (row <= 3)
    for i, s in enumerate(BACK):
        piece = power[s * rows : (s + 1) * rows]
        out_ref[i] = jnp.where(spare & (col == s * rows), term, piece).astype(jnp.bfloat16)


def cross(delayed):
    count, rows, _ = delayed.shape
    vmem = pl.BlockSpec(memory_space=pltpu.VMEM)
    return pl.pallas_call(
        cross_kernel,
        out_shape=jax.ShapeDtypeStruct((count, rows, count * rows), jnp.bfloat16),
        in_specs=[vmem],
        out_specs=vmem,
        compiler_params=pltpu.CompilerParams(vmem_limit_bytes=8 << 20),
        name="cross",
    )(delayed)


def finish_kernel(back_ref, power_ref, band_ref):
    bands, rows, total = back_ref.shape
    start = lax.axis_index("bl") * rows
    power = jnp.stack([back_ref[BACK.index(s)] for s in OUT]).astype(jnp.float32)
    power_ref[...] = power
    lane = lax.broadcasted_iota(jnp.int32, (bands, total), 1)
    top = power[:, 0, :]
    band = jnp.zeros((bands, 1), jnp.float32)
    for i in range(1, 4):
        line = power[:, i, :]
        band += jnp.sum(jnp.where(lane == start, line, 0.0), axis=1, keepdims=True)
        value = jnp.sum(jnp.where(lane == start + i, top, 0.0), axis=1, keepdims=True)
        power_ref[:, i, :] = jnp.where(lane == start, value, line)
    row = lax.broadcasted_iota(jnp.int32, (bands, bands), 0)
    col = lax.broadcasted_iota(jnp.int32, (bands, bands), 1)
    band_ref[...] = jnp.sum(jnp.where(row == col, band, 0.0), axis=0, keepdims=True)


def finish(back):
    bands, rows, total = back.shape
    vmem = pl.BlockSpec(memory_space=pltpu.VMEM)
    return pl.pallas_call(
        finish_kernel,
        out_shape=(
            jax.ShapeDtypeStruct((bands, rows, total), jnp.float32),
            jax.ShapeDtypeStruct((1, bands), jnp.float32),
        ),
        in_specs=[vmem],
        out_specs=(vmem, vmem),
        compiler_params=pltpu.CompilerParams(vmem_limit_bytes=8 << 20),
        name="finish",
    )(back)


def shards(visibilities, flags):
    own = spectra(visibilities, flags)
    mine = lax.all_to_all(own, "bl", 0, 0, tiled=True, axis_index_groups=[OUT])
    back = lax.all_to_all(cross(mine), "bl", 0, 0, tiled=True, axis_index_groups=[BACK])
    power, band = finish(back)
    return (power, band.reshape(-1))


def solution(mesh):
    return jax.shard_map(
        shards,
        mesh=mesh,
        in_specs=(P(None, ("group", "bl"), None, None), P(("group", "bl"), None)),
        out_specs=(P(None, ("group", "bl"), None), P("group")),
        check_vma=False,
    )
```

```python
import math

import jax
import jax.numpy as jnp
import numpy as np
from jax import lax
from jax.experimental import pallas as pl
from jax.experimental.pallas import tpu as pltpu
from jax.sharding import PartitionSpec as P

NF = 1024
NT = 16
CB = 128
BW = 32
NCB = 8
NB = NF // BW
GROUP = 4
HALF_ROOT = math.sqrt(0.5)
OUT = [
    27, 15, 14, 12, 6, 10, 21, 16, 19, 30, 25, 4, 7, 2, 13, 8, 11, 18, 31, 28, 17, 26, 5, 0, 3, 1,
    9, 20, 23, 22, 29, 24,
]
BACK = [(-3 * i % 32) ^ 26 for i in range(32)]


def taper_table():
    angle = np.arange(NF, dtype=np.float64) * (2.0 * math.pi / (NF - 1))
    taper = 0.35875 - 0.48829 * np.cos(angle) + 0.14128 * np.cos(2.0 * angle) - 0.01168 * np.cos(3.0 * angle)
    return taper.reshape(NCB, CB)


def transform_table():
    h = np.arange(128)[:, None]
    g = np.arange(CB)[None, :]
    phi = (h * g % CB) * (2.0 * math.pi / CB)
    scale = 1.0 / math.sqrt(NF)
    cosine, sine = np.cos(phi) * scale, np.sin(phi) * scale
    real = np.concatenate([cosine, sine], 1).reshape(NB, 1, 4, 2 * CB)
    imag = np.concatenate([-sine, cosine], 1).reshape(NB, 1, 4, 2 * CB)
    full = np.concatenate([real, imag], 1).reshape(2 * CB, 2 * CB)
    high = full.astype(jnp.bfloat16)
    low = (full - high.astype(np.float64)).astype(jnp.bfloat16)
    return jnp.asarray(np.stack([high, low]))


def row_table():
    phi = np.arange(8)[:, None] * np.arange(CB)[None, :] * (2.0 * math.pi / NF)
    return jnp.asarray(np.concatenate([taper_table(), np.cos(phi), np.sin(phi)]).astype(np.float32))


def two(a, b):
    return (a[0] + b[0], a[1] + b[1]), (a[0] - b[0], a[1] - b[1])


def four(x0, x1, x2, x3):
    s0, d0 = two(x0, x2)
    s1, d1 = two(x1, x3)
    y0, y2 = two(s0, s1)
    y1, y3 = two(d0, (d1[1], -d1[0]))
    return y0, y1, y2, y3


def eight(x):
    pairs = [two(x[a], x[a + 4]) for a in range(4)]
    d = [p[1] for p in pairs]
    d[1] = ((d[1][0] + d[1][1]) * HALF_ROOT, (d[1][1] - d[1][0]) * HALF_ROOT)
    d[2] = (d[2][1], -d[2][0])
    d[3] = ((d[3][1] - d[3][0]) * HALF_ROOT, (d[3][0] + d[3][1]) * -HALF_ROOT)
    even, odd = four(*(p[0] for p in pairs)), four(*d)
    return [even[0], odd[0], even[1], odd[1], even[2], odd[2], even[3], odd[3]]


def spectra_kernel(x_hbm, flags_hbm, rows_hbm, table_hbm, out_ref, xs, flags_ref, rows_ref, yh, yl, z, table, sems, side_sems):
    rows = flags_ref.shape[1]
    small = [
        pltpu.make_async_copy(flags_hbm, flags_ref, side_sems.at[0]),
        pltpu.make_async_copy(rows_hbm, rows_ref, side_sems.at[1]),
    ]
    copies = [
        pltpu.make_async_copy(x_hbm.at[part, :, t, :], xs.at[part, t], sems.at[part, t])
        for t in range(NT)
        for part in range(2)
    ]
    tables = pltpu.make_async_copy(table_hbm, table, side_sems.at[2])
    for c in [*small, tables, *copies]:
        c.start()
    for c in small:
        c.wait()
    flags = flags_ref[...].astype(jnp.float32).T
    weight = []
    for a in range(NCB):
        keep = jnp.broadcast_to(flags[:, a : a + 1], (rows, CB))
        weight.append(keep * rows_ref[a : a + 1, :])

    def fold(t):
        u = [
            tuple(xs[part, t, :, a * CB : (a + 1) * CB] * weight[a] for part in range(2)) for a in range(NCB)
        ]
        y = eight(u)
        for r in range(8):
            re, im = y[r]
            if r:
                cosine, sine = rows_ref[8 + r : 9 + r, :], rows_ref[16 + r : 17 + r, :]
                re, im = re * cosine + im * sine, im * cosine - re * sine
            at = pl.ds((r * GROUP + t % GROUP) * rows, rows)
            for part, value in enumerate((re, im)):
                high = value.astype(jnp.bfloat16)
                yh[t // GROUP, at, part * CB : (part + 1) * CB] = high
                low = (value - high.astype(jnp.float32)).astype(jnp.bfloat16)
                yl[t // GROUP, at, part * CB : (part + 1) * CB] = low

    def multiply(g):
        width = yh.shape[1]
        dims = (((1,), (1,)), ((), ()))
        z[:, g * width : (g + 1) * width] = (
            lax.dot_general(table[0], yh[g], dims, preferred_element_type=jnp.float32)
            + lax.dot_general(table[1], yh[g], dims, preferred_element_type=jnp.float32)
            + lax.dot_general(table[0], yl[g], dims, preferred_element_type=jnp.float32)
        )

    for g in range(NT // GROUP):
        for c in copies[2 * GROUP * g : 2 * GROUP * (g + 1)]:
            c.wait()
        if g == 1:
            tables.wait()
        if g:
            multiply(g - 1)
        for t in range(g * GROUP, (g + 1) * GROUP):
            fold(t)
    multiply(NT // GROUP - 1)
    for k in range(NB):
        tiles = [z[8 * k : 8 * k + 8, m * 128 : (m + 1) * 128] for m in range(z.shape[1] // 128)]
        block = jnp.concatenate(tiles, 0).T.astype(jnp.bfloat16)
        for i in range(8):
            out_ref[k, :, i * 128 : (i + 1) * 128] = block[i * rows : (i + 1) * rows, :]


def in_hbm(array):
    return pltpu.with_memory_space_constraint(array, pltpu.HBM)


def spectra(visibilities, flags):
    rows = visibilities.shape[1]
    table, row = transform_table(), row_table()
    hbm = pl.BlockSpec(memory_space=pltpu.HBM)
    return pl.pallas_call(
        spectra_kernel,
        out_shape=pltpu.VMEM((NB, rows, NT * 2 * BW), jnp.bfloat16),
        in_specs=[hbm] * 4,
        out_specs=pl.BlockSpec(memory_space=pltpu.VMEM),
        compiler_params=pltpu.CompilerParams(vmem_limit_bytes=24 << 20),
        scratch_shapes=[
            pltpu.VMEM((2, NT, rows, NF), jnp.float32),
            pltpu.VMEM((NCB, rows), jnp.int32),
            pltpu.VMEM(row.shape, jnp.float32),
            pltpu.VMEM((NT // GROUP, 8 * GROUP * rows, 2 * CB), jnp.bfloat16),
            pltpu.VMEM((NT // GROUP, 8 * GROUP * rows, 2 * CB), jnp.bfloat16),
            pltpu.VMEM((2 * CB, 8 * NT * rows), jnp.float32),
            pltpu.VMEM(table.shape, jnp.bfloat16),
            pltpu.SemaphoreType.DMA((2, NT)),
            pltpu.SemaphoreType.DMA((3,)),
        ],
        name="spectra",
    )(in_hbm(visibilities), in_hbm(flags.T), in_hbm(row), in_hbm(table))


def cross_kernel(own_ref, out_ref):
    count, rows, _ = out_ref.shape
    total = count * rows
    delayed = jnp.concatenate([own_ref[OUT.index(s)] for s in range(count)], 0)
    power = lax.dot_general(
        delayed, delayed, (((1,), (1,)), ((), ())), preferred_element_type=jnp.float32
    ) * (1.0 / NT)
    out_ref[:, :, 0:total] = power.astype(jnp.bfloat16).reshape(count, rows, total)
    row = lax.broadcasted_iota(jnp.int32, (total, total), 0)
    col = lax.broadcasted_iota(jnp.int32, (total, total), 1)
    off = jnp.where(row == col, 0.0, power)
    band = jnp.sum(jnp.sum(off, axis=0, keepdims=True), axis=1, keepdims=True) * (1.0 / total)
    band = jnp.broadcast_to(band, (rows, total))
    first = band.astype(jnp.bfloat16).astype(jnp.float32)
    second = (band - first).astype(jnp.bfloat16).astype(jnp.float32)
    third = band - first - second
    row = lax.broadcasted_iota(jnp.int32, (rows, total), 0)
    col = lax.broadcasted_iota(jnp.int32, (rows, total), 1)
    term = jnp.where(row == 1, first, jnp.where(row == 2, second, third))
    spare = (row >= 1) & (row <= 3)
    for i, s in enumerate(BACK):
        piece = power[s * rows : (s + 1) * rows]
        out_ref[i] = jnp.where(spare & (col == s * rows), term, piece).astype(jnp.bfloat16)


def cross(delayed):
    count, rows, _ = delayed.shape
    vmem = pl.BlockSpec(memory_space=pltpu.VMEM)
    return pl.pallas_call(
        cross_kernel,
        out_shape=jax.ShapeDtypeStruct((count, rows, count * rows), jnp.bfloat16),
        in_specs=[vmem],
        out_specs=vmem,
        compiler_params=pltpu.CompilerParams(vmem_limit_bytes=8 << 20),
        name="cross",
    )(delayed)


def finish_kernel(back_ref, power_ref, band_ref):
    bands, rows, total = back_ref.shape
    start = lax.axis_index("bl") * rows
    power = jnp.stack([back_ref[BACK.index(s)] for s in OUT]).astype(jnp.float32)
    power_ref[...] = power
    lane = lax.broadcasted_iota(jnp.int32, (bands, total), 1)
    top = power[:, 0, :]
    band = jnp.zeros((bands, 1), jnp.float32)
    for i in range(1, 4):
        line = power[:, i, :]
        band += jnp.sum(jnp.where(lane == start, line, 0.0), axis=1, keepdims=True)
        value = jnp.sum(jnp.where(lane == start + i, top, 0.0), axis=1, keepdims=True)
        power_ref[:, i, :] = jnp.where(lane == start, value, line)
    row = lax.broadcasted_iota(jnp.int32, (bands, bands), 0)
    col = lax.broadcasted_iota(jnp.int32, (bands, bands), 1)
    band_ref[...] = jnp.sum(jnp.where(row == col, band, 0.0), axis=0, keepdims=True)


def finish(back):
    bands, rows, total = back.shape
    vmem = pl.BlockSpec(memory_space=pltpu.VMEM)
    return pl.pallas_call(
        finish_kernel,
        out_shape=(
            jax.ShapeDtypeStruct((bands, rows, total), jnp.float32),
            jax.ShapeDtypeStruct((1, bands), jnp.float32),
        ),
        in_specs=[vmem],
        out_specs=(vmem, vmem),
        compiler_params=pltpu.CompilerParams(vmem_limit_bytes=8 << 20),
        name="finish",
    )(back)


def shards(visibilities, flags):
    own = spectra(visibilities, flags)
    mine = lax.all_to_all(own, "bl", 0, 0, tiled=True, axis_index_groups=[OUT])
    back = lax.all_to_all(cross(mine), "bl", 0, 0, tiled=True, axis_index_groups=[BACK])
    power, band = finish(back)
    return (power, band.reshape(-1))


def solution(mesh):
    return jax.shard_map(
        shards,
        mesh=mesh,
        in_specs=(P(None, ("group", "bl"), None, None), P(("group", "bl"), None)),
        out_specs=(P(None, ("group", "bl"), None), P("group")),
        check_vma=False,
    )
```

```python
import math

import jax
import jax.numpy as jnp
import numpy as np
from jax import lax
from jax.experimental import pallas as pl
from jax.experimental.pallas import tpu as pltpu
from jax.sharding import PartitionSpec as P

NF = 1024
NT = 16
CB = 128
BW = 32
NCB = 8
NB = NF // BW
GROUP = 4
HALF_ROOT = math.sqrt(0.5)
OUT = [
    27, 15, 14, 12, 6, 10, 21, 16, 19, 30, 25, 4, 7, 2, 13, 8, 11, 18, 31, 28, 17, 26, 5, 0, 3, 1,
    9, 20, 23, 22, 29, 24,
]
BACK = [
    26, 13, 0, 19, 6, 25, 12, 31, 18, 5, 24, 11, 30, 17, 4, 23, 10, 29, 16, 3, 22, 9, 28, 15, 2, 21,
    8, 27, 14, 1, 20, 7,
]


def taper_table():
    angle = np.arange(NF, dtype=np.float64) * (2.0 * math.pi / (NF - 1))
    taper = 0.35875 - 0.48829 * np.cos(angle) + 0.14128 * np.cos(2.0 * angle) - 0.01168 * np.cos(3.0 * angle)
    return taper.reshape(NCB, CB)


def transform_table():
    h = np.arange(128)[:, None]
    g = np.arange(CB)[None, :]
    phi = (h * g % CB) * (2.0 * math.pi / CB)
    scale = 1.0 / math.sqrt(NF)
    cosine, sine = np.cos(phi) * scale, np.sin(phi) * scale
    real = np.concatenate([cosine, sine], 1).reshape(NB, 1, 4, 2 * CB)
    imag = np.concatenate([-sine, cosine], 1).reshape(NB, 1, 4, 2 * CB)
    full = np.concatenate([real, imag], 1).reshape(2 * CB, 2 * CB)
    high = full.astype(jnp.bfloat16)
    low = (full - high.astype(np.float64)).astype(jnp.bfloat16)
    return jnp.asarray(np.stack([high, low]))


def row_table():
    phi = np.arange(8)[:, None] * np.arange(CB)[None, :] * (2.0 * math.pi / NF)
    return jnp.asarray(np.concatenate([taper_table(), np.cos(phi), np.sin(phi)]).astype(np.float32))


def two(a, b):
    return (a[0] + b[0], a[1] + b[1]), (a[0] - b[0], a[1] - b[1])


def four(x0, x1, x2, x3):
    s0, d0 = two(x0, x2)
    s1, d1 = two(x1, x3)
    y0, y2 = two(s0, s1)
    y1, y3 = two(d0, (d1[1], -d1[0]))
    return y0, y1, y2, y3


def eight(x):
    pairs = [two(x[a], x[a + 4]) for a in range(4)]
    d = [p[1] for p in pairs]
    d[1] = ((d[1][0] + d[1][1]) * HALF_ROOT, (d[1][1] - d[1][0]) * HALF_ROOT)
    d[2] = (d[2][1], -d[2][0])
    d[3] = ((d[3][1] - d[3][0]) * HALF_ROOT, (d[3][0] + d[3][1]) * -HALF_ROOT)
    even, odd = four(*(p[0] for p in pairs)), four(*d)
    return [even[0], odd[0], even[1], odd[1], even[2], odd[2], even[3], odd[3]]


def spectra_kernel(x_hbm, flags_hbm, rows_hbm, table_hbm, out_ref, xs, flags_ref, rows_ref, yh, yl, z, table, sems, side_sems):
    rows = flags_ref.shape[1]
    small = [
        pltpu.make_async_copy(flags_hbm, flags_ref, side_sems.at[0]),
        pltpu.make_async_copy(rows_hbm, rows_ref, side_sems.at[1]),
    ]
    copies = [
        pltpu.make_async_copy(x_hbm.at[part, :, t, :], xs.at[part, t], sems.at[part, t])
        for t in range(NT)
        for part in range(2)
    ]
    tables = pltpu.make_async_copy(table_hbm, table, side_sems.at[2])
    for c in [*small, tables, *copies]:
        c.start()
    for c in small:
        c.wait()
    flags = flags_ref[...].astype(jnp.float32).T
    weight = []
    for a in range(NCB):
        keep = jnp.broadcast_to(flags[:, a : a + 1], (rows, CB))
        weight.append(keep * rows_ref[a : a + 1, :])

    def fold(t):
        u = [
            tuple(xs[part, t, :, a * CB : (a + 1) * CB] * weight[a] for part in range(2)) for a in range(NCB)
        ]
        y = eight(u)
        for r in range(8):
            re, im = y[r]
            if r:
                cosine, sine = rows_ref[8 + r : 9 + r, :], rows_ref[16 + r : 17 + r, :]
                re, im = re * cosine + im * sine, im * cosine - re * sine
            at = pl.ds((r * GROUP + t % GROUP) * rows, rows)
            for part, value in enumerate((re, im)):
                high = value.astype(jnp.bfloat16)
                yh[t // GROUP, at, part * CB : (part + 1) * CB] = high
                low = (value - high.astype(jnp.float32)).astype(jnp.bfloat16)
                yl[t // GROUP, at, part * CB : (part + 1) * CB] = low

    def multiply(g):
        width = yh.shape[1]
        dims = (((1,), (1,)), ((), ()))
        z[:, g * width : (g + 1) * width] = (
            lax.dot_general(table[0], yh[g], dims, preferred_element_type=jnp.float32)
            + lax.dot_general(table[1], yh[g], dims, preferred_element_type=jnp.float32)
            + lax.dot_general(table[0], yl[g], dims, preferred_element_type=jnp.float32)
        )

    for g in range(NT // GROUP):
        for c in copies[2 * GROUP * g : 2 * GROUP * (g + 1)]:
            c.wait()
        if g == 1:
            tables.wait()
        for t in range(g * GROUP, (g + 1) * GROUP):
            fold(t)
        if g:
            multiply(g - 1)
    multiply(NT // GROUP - 1)
    for k in range(NB):
        tiles = [z[8 * k : 8 * k + 8, m * 128 : (m + 1) * 128] for m in range(z.shape[1] // 128)]
        block = jnp.concatenate(tiles, 0).T.astype(jnp.bfloat16)
        for i in range(8):
            out_ref[k, :, i * 128 : (i + 1) * 128] = block[i * rows : (i + 1) * rows, :]


def in_hbm(array):
    return pltpu.with_memory_space_constraint(array, pltpu.HBM)


def spectra(visibilities, flags):
    rows = visibilities.shape[1]
    table, row = transform_table(), row_table()
    hbm = pl.BlockSpec(memory_space=pltpu.HBM)
    return pl.pallas_call(
        spectra_kernel,
        out_shape=pltpu.VMEM((NB, rows, NT * 2 * BW), jnp.bfloat16),
        in_specs=[hbm] * 4,
        out_specs=pl.BlockSpec(memory_space=pltpu.VMEM),
        compiler_params=pltpu.CompilerParams(vmem_limit_bytes=24 << 20),
        scratch_shapes=[
            pltpu.VMEM((2, NT, rows, NF), jnp.float32),
            pltpu.VMEM((NCB, rows), jnp.int32),
            pltpu.VMEM(row.shape, jnp.float32),
            pltpu.VMEM((NT // GROUP, 8 * GROUP * rows, 2 * CB), jnp.bfloat16),
            pltpu.VMEM((NT // GROUP, 8 * GROUP * rows, 2 * CB), jnp.bfloat16),
            pltpu.VMEM((2 * CB, 8 * NT * rows), jnp.float32),
            pltpu.VMEM(table.shape, jnp.bfloat16),
            pltpu.SemaphoreType.DMA((2, NT)),
            pltpu.SemaphoreType.DMA((3,)),
        ],
        name="spectra",
    )(in_hbm(visibilities), in_hbm(flags.T), in_hbm(row), in_hbm(table))


def cross_kernel(own_ref, out_ref):
    count, rows, _ = out_ref.shape
    total = count * rows
    delayed = jnp.concatenate([own_ref[OUT.index(s)] for s in range(count)], 0)
    half, dims = total // 2, (((1,), (1,)), ((), ()))
    top = lax.dot_general(delayed[:half], delayed, dims, preferred_element_type=jnp.float32)
    corner = lax.dot_general(delayed[half:], delayed[half:], dims, preferred_element_type=jnp.float32)
    below = jnp.concatenate([top[:, half:].T, corner], 1)
    power = jnp.concatenate([top, below], 0) * (1.0 / NT)
    out_ref[:, :, 0:total] = power.astype(jnp.bfloat16).reshape(count, rows, total)
    row = lax.broadcasted_iota(jnp.int32, (total, total), 0)
    col = lax.broadcasted_iota(jnp.int32, (total, total), 1)
    off = jnp.where(row == col, 0.0, power)
    band = jnp.sum(jnp.sum(off, axis=0, keepdims=True), axis=1, keepdims=True) * (1.0 / total)
    band = jnp.broadcast_to(band, (rows, total))
    first = band.astype(jnp.bfloat16).astype(jnp.float32)
    second = (band - first).astype(jnp.bfloat16).astype(jnp.float32)
    third = band - first - second
    row = lax.broadcasted_iota(jnp.int32, (rows, total), 0)
    col = lax.broadcasted_iota(jnp.int32, (rows, total), 1)
    term = jnp.where(row == 1, first, jnp.where(row == 2, second, third))
    spare = (row >= 1) & (row <= 3)
    for i, s in enumerate(BACK):
        piece = power[s * rows : (s + 1) * rows]
        out_ref[i] = jnp.where(spare & (col == s * rows), term, piece).astype(jnp.bfloat16)


def cross(delayed):
    count, rows, _ = delayed.shape
    vmem = pl.BlockSpec(memory_space=pltpu.VMEM)
    return pl.pallas_call(
        cross_kernel,
        out_shape=jax.ShapeDtypeStruct((count, rows, count * rows), jnp.bfloat16),
        in_specs=[vmem],
        out_specs=vmem,
        compiler_params=pltpu.CompilerParams(vmem_limit_bytes=8 << 20),
        name="cross",
    )(delayed)


def finish_kernel(back_ref, power_ref, band_ref):
    bands, rows, total = back_ref.shape
    start = lax.axis_index("bl") * rows
    power = jnp.stack([back_ref[BACK.index(s)] for s in OUT]).astype(jnp.float32)
    power_ref[...] = power
    lane = lax.broadcasted_iota(jnp.int32, (bands, total), 1)
    top = power[:, 0, :]
    band = jnp.zeros((bands, 1), jnp.float32)
    for i in range(1, 4):
        line = power[:, i, :]
        band += jnp.sum(jnp.where(lane == start, line, 0.0), axis=1, keepdims=True)
        value = jnp.sum(jnp.where(lane == start + i, top, 0.0), axis=1, keepdims=True)
        power_ref[:, i, :] = jnp.where(lane == start, value, line)
    row = lax.broadcasted_iota(jnp.int32, (bands, bands), 0)
    col = lax.broadcasted_iota(jnp.int32, (bands, bands), 1)
    band_ref[...] = jnp.sum(jnp.where(row == col, band, 0.0), axis=0, keepdims=True)


def finish(back):
    bands, rows, total = back.shape
    vmem = pl.BlockSpec(memory_space=pltpu.VMEM)
    return pl.pallas_call(
        finish_kernel,
        out_shape=(
            jax.ShapeDtypeStruct((bands, rows, total), jnp.float32),
            jax.ShapeDtypeStruct((1, bands), jnp.float32),
        ),
        in_specs=[vmem],
        out_specs=(vmem, vmem),
        compiler_params=pltpu.CompilerParams(vmem_limit_bytes=8 << 20),
        name="finish",
    )(back)


def shards(visibilities, flags):
    own = spectra(visibilities, flags)
    mine = lax.all_to_all(own, "bl", 0, 0, tiled=True, axis_index_groups=[OUT])
    back = lax.all_to_all(cross(mine), "bl", 0, 0, tiled=True, axis_index_groups=[BACK])
    power, band = finish(back)
    return (power, band.reshape(-1))


def solution(mesh):
    return jax.shard_map(
        shards,
        mesh=mesh,
        in_specs=(P(None, ("group", "bl"), None, None), P(("group", "bl"), None)),
        out_specs=(P(None, ("group", "bl"), None), P("group")),
        check_vma=False,
    )
```
